32 devices in a mesh: dp: 2 (over z, core), tp: 16 (over x, y).
Axes of the slice: x: 4, y: 4, z: 1, core: 2. Of those that a mesh axis runs over, the one named last changes fastest.
The devices are a block of a 4x4x4 slice.
Arguments:
- x: bfloat16 [128, 8192], P('dp'), parts along dimension 0
- k_cache: bfloat16 [128, 1024, 64, 128], P('dp', None, 'tp'), parts along dimension 0
- v_cache: bfloat16 [128, 1024, 64, 128], P('dp', None, 'tp'), parts along dimension 0
- gain_a: bfloat16 [8192], replicated
- wq: bfloat16 [8192, 8192], P(None, 'tp')
- wo: bfloat16 [8192, 8192], P('tp')
- gain_m: bfloat16 [8192], replicated
- w_gate: bfloat16 [8192, 24576], P(None, 'tp')
- w_up: bfloat16 [8192, 24576], P(None, 'tp')
- w_down: bfloat16 [24576, 8192], P('tp')
Outputs:
- output: bfloat16 [128, 8192], P('dp'), parts along dimension 0
There are 2 independent parts. The reference program is written for one: setup_inputs(seed, part) draws one part's arguments, and reference() takes and returns one part's arrays. A program takes and returns all parts, laid end to end along the dimension named above; an argument that names none is the same for every part.
All inputs are finite; a program needn't handle non-finite values.
Results may differ from the reference program's by a relative error of at most 0.017.
Values are sent between devices in bfloat16 or wider.
A program may use at most 1.5 GiB of HBM per device.

```python
import jax
import jax.numpy as jnp
from jax import lax

BATCH = 64
CACHE = 1024
D = 8192
HEADS = 64
KV_HEADS = 64
HEAD = 128
FF = 24576
THETA = 10000


def setup_inputs(seed: int = 0, part: int = 0) -> dict:
    kx, kc, kw, kn, kq, ko, km, kg, ku, kd = jax.random.split(jax.random.key(seed), 10)
    kx, kc, kw = (jax.random.fold_in(k, part) for k in (kx, kc, kw))

    def weights(key, rows, columns):
        return jax.random.normal(key, (rows, columns), jnp.float32) * rows**-0.5

    drawn = {
        "x": jax.random.normal(kx, (BATCH, D), jnp.float32),
        "k_cache": 2 * jax.random.normal(kc, (BATCH, CACHE, KV_HEADS, HEAD), jnp.float32),
        "v_cache": 4 * jax.random.normal(kw, (BATCH, CACHE, KV_HEADS, HEAD), jnp.float32),
        "gain_a": 1 + 0.1 * jax.random.normal(kn, (D,), jnp.float32),
        "wq": 2 * weights(kq, D, HEADS * HEAD),
        "wo": weights(ko, HEADS * HEAD, D),
        "gain_m": 1 + 0.1 * jax.random.normal(km, (D,), jnp.float32),
        "w_gate": weights(kg, D, FF),
        "w_up": weights(ku, D, FF),
        "w_down": 2 * weights(kd, FF, D),
    }
    return {k: v.astype(jnp.bfloat16) for k, v in drawn.items()}


def normed(x, gain):
    wide = x.astype(jnp.float32)
    scale = lax.rsqrt(jnp.mean(wide * wide, -1, keepdims=True) + 1e-6)
    return (wide * scale * gain.astype(jnp.float32)).astype(jnp.bfloat16)


def turned(t, place, theta):
    half = t.shape[-1] // 2
    angle = place.astype(jnp.float32)[:, None] * theta ** (-jnp.arange(half, dtype=jnp.float32) / half)
    cos, sin = jnp.cos(angle)[:, None], jnp.sin(angle)[:, None]
    a, b = t[..., :half].astype(jnp.float32), t[..., half:].astype(jnp.float32)
    return jnp.concatenate([a * cos - b * sin, b * cos + a * sin], -1).astype(jnp.bfloat16)


def matmul(a, w):
    return jnp.dot(a, w, preferred_element_type=jnp.float32).astype(jnp.bfloat16)


def einsum(form, a, b):
    return jnp.einsum(form, a.astype(jnp.float32), b.astype(jnp.float32))


def seen_by(a, wq, k_cache, v_cache, head, theta):
    batch, cache, kv_heads = k_cache.shape[:3]
    place = jnp.full((batch,), cache - 1)
    q = turned(matmul(a, wq).reshape(batch, -1, head), place, theta).reshape(batch, kv_heads, -1, head)
    scores = einsum("bgsd,bugd->bgsu", q, k_cache) * head**-0.5
    weights = jax.nn.softmax(scores, -1).astype(jnp.bfloat16)
    return einsum("bgsu,bugd->bgsd", weights, v_cache).astype(jnp.bfloat16).reshape(batch, -1)


def hidden_of(b, w_gate, w_up):
    gate = jnp.dot(b, w_gate, preferred_element_type=jnp.float32)
    up = jnp.dot(b, w_up, preferred_element_type=jnp.float32)
    return (jax.nn.silu(gate) * up).astype(jnp.bfloat16)


def reference(x, k_cache, v_cache, gain_a, wq, wo, gain_m, w_gate, w_up, w_down):
    seen = seen_by(normed(x, gain_a), wq, k_cache, v_cache, HEAD, THETA)
    h = (x.astype(jnp.float32) + jnp.dot(seen, wo, preferred_element_type=jnp.float32)).astype(jnp.bfloat16)
    hidden = hidden_of(normed(h, gain_m), w_gate, w_up)
    return (h.astype(jnp.float32) + jnp.dot(hidden, w_down, preferred_element_type=jnp.float32)).astype(jnp.bfloat16)
```

```python
import functools
import math

import jax
import jax.numpy as jnp
from jax import lax
from jax.experimental import pallas as pl
from jax.experimental.pallas import tpu as pltpu
from jax.sharding import PartitionSpec as P

HEAD = 128
THETA = 10000
BF16, F32 = jnp.bfloat16, jnp.float32
MESH = pl.DeviceIdType.MESH
SLOTS = 4
FAR_FIRST = (2, 1, 3)


def normed(x, gain):
    wide = x.astype(jnp.float32)
    scale = lax.rsqrt(jnp.mean(wide * wide, -1, keepdims=True) + 1e-6)
    return (wide * scale * gain.astype(jnp.float32)).astype(jnp.bfloat16)


def turned(t, place, theta):
    half = t.shape[-1] // 2
    angle = place.astype(jnp.float32)[:, None] * theta ** (-jnp.arange(half, dtype=jnp.float32) / half)
    cos, sin = jnp.cos(angle)[:, None], jnp.sin(angle)[:, None]
    a, b = t[..., :half].astype(jnp.float32), t[..., half:].astype(jnp.float32)
    return jnp.concatenate([a * cos - b * sin, b * cos + a * sin], -1).astype(jnp.bfloat16)


def matmul(a, w):
    return jnp.dot(a, w, preferred_element_type=jnp.float32).astype(jnp.bfloat16)


def einsum(form, a, b):
    return jnp.einsum(form, a.astype(jnp.float32), b.astype(jnp.float32))


def seen_by(a, wq, k_cache, v_cache, head, theta):
    batch, cache, kv_heads = k_cache.shape[:3]
    place = jnp.full((batch,), cache - 1)
    q = turned(matmul(a, wq).reshape(batch, -1, head), place, theta).reshape(batch, kv_heads, -1, head)
    scores = einsum("bgsd,bugd->bgsu", q, k_cache) * head**-0.5
    weights = jax.nn.softmax(scores, -1).astype(jnp.bfloat16)
    return einsum("bgsu,bugd->bgsd", weights, v_cache).astype(jnp.bfloat16).reshape(batch, -1)


def dot(a, w):
    return jnp.dot(a, w, preferred_element_type=F32)


def tail_kernel(side, seen, x, gain, wo, w_gate, w_up, w_down, out, wg, wu, dn, xp, hp, term, own1, got1, sent2, own2, got2, ag, b, gacc, uacc, hid,
                x_sem, wo_sem, g_sem, u_sem, d_sem, s1, r1, s2, r2, sv, rv, su, ru):
    me = lax.axis_index("tp")
    at = (me // side, me % side)
    rows, depth = seen.shape
    d, ff = w_gate.shape
    wide = d // (2 * side)
    w = wide // side
    bk = depth
    bn = wide // 2
    nk = d // bk
    order = FAR_FIRST + (0,)
    steps = [(g, h) for g in order for h in range(2)]

    def peer(axis, g):
        place = [at[0], at[1]]
        place[axis] = lax.rem(at[axis] + g, side)
        return {"tp": place[0] * side + place[1]}

    def first_column(h, g):
        return pl.multiple_of((h * side + lax.rem(at[h] + g, side)) * wide, wide)

    across = ff // bn
    wo_rows = -(-2 * len(steps) // across)

    def wo_piece(j):
        g, h = steps[j // 2]
        home = wu.at[pl.ds((nk - wo_rows + j // across) * bk, bk), pl.ds((j % across) * bn, bn)]
        return pltpu.make_async_copy(wo.at[:, pl.ds(pl.multiple_of(first_column(h, g) + (j % 2) * bn, bn), bn)], home, wo_sem.at[j]), home

    def gate_piece(k):
        part = pl.ds(pl.multiple_of(k * bk, bk), bk)
        return pltpu.make_async_copy(w_gate.at[part, :], wg.at[part, :], g_sem.at[k])

    def up_piece(k):
        part = pl.ds(pl.multiple_of(k * bk, bk), bk)
        return pltpu.make_async_copy(w_up.at[part, :], wu.at[part, :], u_sem.at[k])

    def down_piece(j):
        g, h = steps[j // 2]
        return pltpu.make_async_copy(w_down.at[:, pl.ds(pl.multiple_of(first_column(h, g) + (j % 2) * bn, bn), bn)], dn.at[j % SLOTS], d_sem.at[j % SLOTS])

    def x_piece(h):
        return pltpu.make_async_copy(x.at[:, pl.ds(pl.multiple_of(first_column(h, 0) + at[1 - h] * w, w), w)], xp.at[h], x_sem.at[h])

    barrier = pltpu.get_barrier_semaphore()
    for axis in range(2):
        for g in range(1, side):
            pl.semaphore_signal(barrier, inc=1, device_id=peer(axis, g), device_id_type=MESH)
    for j in range(2 * len(steps)):
        wo_piece(j)[0].start()
    for h in range(2):
        x_piece(h).start()
    for k in range(nk):
        gate_piece(k).start()
        if k < nk - wo_rows:
            up_piece(k).start()
    for j in range(SLOTS):
        down_piece(j).start()
    pl.semaphore_wait(barrier, 2 * (side - 1))

    def summed(piece, base):
        firsts, seconds, copies = [], [], []
        for i, (g, h) in enumerate(steps):
            for c in range(2):
                value = piece(2 * i + c)
                if g:
                    term[h, g - 1, :, pl.ds(c * bn, bn)] = value.astype(BF16)
                else:
                    own1[h, :, pl.ds(c * bn, bn)] = value
            if g:
                copy = pltpu.make_async_remote_copy(term.at[h, g - 1], got1.at[h, g - 1], s1.at[h, g - 1], r1.at[h, g - 1], device_id=peer(h, g), device_id_type=MESH)
                copy.start()
                firsts.append((h, copy))
        for h in range(2):
            for half, copy in firsts:
                if half == h:
                    copy.wait_recv()
            for g in order:
                part = pl.ds(pl.multiple_of(lax.rem(at[1 - h] + g, side) * w, w), w)
                total = own1[h, :, part]
                for k in range(side - 1):
                    total += got1[h, k, :, part].astype(F32)
                if g:
                    sent2[h, g - 1] = total.astype(BF16)
                    copy = pltpu.make_async_remote_copy(sent2.at[h, g - 1], got2.at[h, g - 1], s2.at[h, g - 1], r2.at[h, g - 1], device_id=peer(1 - h, g), device_id_type=MESH)
                    copy.start()
                    seconds.append((h, copy))
                else:
                    own2[h] = total
        news, arrivals = {}, []
        for h in range(2):
            for half, copy in seconds:
                if half == h:
                    copy.wait_recv()
            total = own2[h]
            for k in range(side - 1):
                total += got2[h, k].astype(F32)
            value = (base(h) + total).astype(BF16)
            hp[h] = value
            mine = ag.at[h, at[h], at[1 - h]]
            mine[...] = value
            for g in FAR_FIRST:
                copy = pltpu.make_async_remote_copy(mine, mine, sv.at[h, g - 1], rv.at[h, g - 1], device_id=peer(1 - h, g), device_id_type=MESH)
                copy.start()
                news[h, g] = copy
                copies.append(copy)
            for g in FAR_FIRST:
                copy = pltpu.make_async_remote_copy(mine, mine, su.at[h, g - 1, 0], ru.at[h, g - 1, 0], device_id=peer(h, g), device_id_type=MESH)
                copy.start()
                copies.append(copy)
                arrivals.append(copy)
        for k in (1, 3, 2):
            for h in range(2):
                news[h, k].wait_recv()
                came = ag.at[h, at[h], lax.rem(at[1 - h] + side - k, side)]
                for g in FAR_FIRST:
                    copy = pltpu.make_async_remote_copy(came, came, su.at[h, g - 1, k], ru.at[h, g - 1, k], device_id=peer(h, g), device_id_type=MESH)
                    copy.start()
                    copies.append(copy)
                    arrivals.append(copy)
        for copy in arrivals:
            copy.wait_recv()
        for _, copy in firsts + seconds:
            copy.wait_send()
        for copy in copies:
            copy.wait_send()

    def attention_term(j):
        copy, home = wo_piece(j)
        copy.wait()
        value = dot(seen[...], home[...])
        if j % across == across - 1 or j == 2 * len(steps) - 1:
            up_piece(nk - wo_rows + j // across).start()
        return value

    def of_x(h):
        x_piece(h).wait()
        return xp[h].astype(F32)

    summed(attention_term, of_x)

    squares = jnp.zeros((rows, w), F32)
    blocks = [(h, u, v) for h in range(2) for u in range(side) for v in range(side)]
    for h, u, v in blocks:
        value = ag[h, u, v].astype(F32)
        squares += value * value
    scale = lax.rsqrt(jnp.sum(squares, -1, keepdims=True) / d + 1e-6)
    for i, (h, u, v) in enumerate(blocks):
        part = pl.ds(i * w, w)
        b[:, part] = (ag[h, u, v].astype(F32) * scale * gain[:, part].astype(F32)).astype(BF16)

    gacc[...] = jnp.zeros_like(gacc)
    uacc[...] = jnp.zeros_like(uacc)

    @pl.loop(0, nk)
    def _(k):
        part = pl.ds(pl.multiple_of(k * bk, bk), bk)
        gate_piece(k).wait()
        gacc[...] += dot(b[:, part], wg[part, :])
        up_piece(k).wait()
        uacc[...] += dot(b[:, part], wu[part, :])

    gate = gacc[...]
    hid[...] = (gate * jax.nn.sigmoid(gate) * uacc[...]).astype(BF16)

    def mlp_term(j):
        down_piece(j).wait()
        value = dot(hid[...], dn[j % SLOTS])
        if j + SLOTS < 2 * len(steps):
            down_piece(j + SLOTS).start()
        return value

    summed(mlp_term, lambda h: hp[h].astype(F32))
    for i, (h, u, v) in enumerate(blocks):
        out[:, pl.ds(i * w, w)] = ag[h, u, v]


def tail(side, seen, x, gain, wo, w_gate, w_up, w_down):
    rows, depth = seen.shape
    d, ff = w_gate.shape
    wide = d // (2 * side)
    w = wide // side
    nk = d // depth
    hops = side - 1
    hbm, vmem, dma = pl.BlockSpec(memory_space=pl.ANY), pl.BlockSpec(memory_space=pltpu.VMEM), pltpu.SemaphoreType.DMA
    return pl.pallas_call(
        functools.partial(tail_kernel, side),
        out_shape=jax.ShapeDtypeStruct((rows, d), BF16),
        in_specs=[vmem, hbm, vmem, hbm, hbm, hbm, hbm],
        out_specs=vmem,
        scratch_shapes=[
            pltpu.VMEM((d, ff), BF16),
            pltpu.VMEM((d, ff), BF16),
            pltpu.VMEM((SLOTS, ff, wide // 2), BF16),
            pltpu.VMEM((2, rows, w), BF16),
            pltpu.VMEM((2, rows, w), BF16),
            pltpu.VMEM((2, hops, rows, wide), BF16),
            pltpu.VMEM((2, rows, wide), F32),
            pltpu.VMEM((2, hops, rows, wide), BF16),
            pltpu.VMEM((2, hops, rows, w), BF16),
            pltpu.VMEM((2, rows, w), F32),
            pltpu.VMEM((2, hops, rows, w), BF16),
            pltpu.VMEM((2, side, side, rows, w), BF16),
            pltpu.VMEM((rows, d), BF16),
            pltpu.VMEM((rows, ff), F32),
            pltpu.VMEM((rows, ff), F32),
            pltpu.VMEM((rows, ff), BF16),
            dma((2,)),
            dma((4 * side,)),
            dma((nk,)),
            dma((nk,)),
            dma((SLOTS,)),
            dma((2, hops)),
            dma((2, hops)),
            dma((2, hops)),
            dma((2, hops)),
            dma((2, hops)),
            dma((2, hops)),
            dma((2, hops, side)),
            dma((2, hops, side)),
        ],
        compiler_params=pltpu.CompilerParams(collective_id=0, has_side_effects=True, vmem_limit_bytes=67043328),
    )(seen, x, gain.reshape(1, d), wo, w_gate, w_up, w_down)


def solution(mesh):
    side = math.isqrt(mesh.shape["tp"])

    def step(x, k_cache, v_cache, gain_a, wq, wo, gain_m, w_gate, w_up, w_down):
        seen = seen_by(normed(x, gain_a), wq, k_cache, v_cache, HEAD, THETA)
        return tail(side, seen, x, gain_m, wo, w_gate, w_up, w_down)

    states, cache, columns, rows_of = P("dp", None), P("dp", None, "tp", None), P(None, "tp"), P("tp", None)
    return jax.shard_map(
        step,
        mesh=mesh,
        in_specs=(states, cache, cache, P(None), columns, rows_of, P(None), columns, columns, rows_of),
        out_specs=states,
        check_vma=False,
    )
```

```python
import functools
import math

import jax
import jax.numpy as jnp
import numpy as np
from jax import lax
from jax.experimental import pallas as pl
from jax.experimental.pallas import tpu as pltpu
from jax.sharding import PartitionSpec as P

THETA = 10000
BF16, F32 = jnp.bfloat16, jnp.float32
MESH = pl.DeviceIdType.MESH
SLOTS = 4
KV_SLOTS = 12
GROUP = 4
FIRST = 2
JOINT = 4
FAR_FIRST = (2, 1, 3)


def dot(a, w):
    return jnp.dot(a, w, preferred_element_type=F32)


def head_kernel(heads, x, gain, cos, sin, wq, k, v, seen, xv, a, wqv, kb, vb, gf, qs, os, sc0, sc1, x_sem, w_sem, k_sem, v_sem):
    rows, d = x.shape
    head = k.shape[1]
    span = k.shape[0] // rows
    slots = kb.shape[0]
    bk = wqv.shape[0] // w_sem.shape[0]
    scale = head**-0.5
    scores = (sc0, sc1)

    def k_piece(s):
        return pltpu.make_async_copy(k.at[pl.ds(pl.multiple_of(s * span, span), span), :], kb.at[lax.rem(s, slots)], k_sem.at[lax.rem(s, slots)])

    def v_piece(s):
        return pltpu.make_async_copy(v.at[pl.ds(pl.multiple_of(s * span, span), span), :], vb.at[lax.rem(s, slots)], v_sem.at[lax.rem(s, slots)])

    def w_piece(i):
        return pltpu.make_async_copy(wq.at[pl.ds(i * bk, bk), :], wqv.at[pl.ds(i * bk, bk), :], w_sem.at[i])

    fetch_x = pltpu.make_async_copy(x, xv, x_sem)
    fetch_x.start()
    fetch_x.wait()
    for i in range(w_sem.shape[0]):
        w_piece(i).start()
    for s in range(FIRST):
        k_piece(s).start()
        v_piece(s).start()
    gf[...] = gain[...].astype(F32)
    qs[...] = jnp.zeros_like(qs)
    squares = jnp.zeros((rows, 128), F32)
    for i in range(d // 128):
        value = xv[:, pl.ds(i * 128, 128)].astype(F32)
        squares += value * value
    norm = lax.rsqrt(jnp.sum(squares, -1, keepdims=True) / d + 1e-6)
    for i in range(d // 128):
        part = pl.ds(i * 128, 128)
        a[:, part] = (xv[:, part].astype(F32) * norm * gf[pl.ds(i, 1), :]).astype(BF16)
    q = jnp.zeros((rows, heads * head), F32)
    for i in range(w_sem.shape[0]):
        if i == w_sem.shape[0] // 2:
            for s in range(FIRST, slots):
                k_piece(s).start()
                v_piece(s).start()
        w_piece(i).wait()
        q += dot(a[:, pl.ds(i * bk, bk)], wqv[pl.ds(i * bk, bk), :])
    q = q.astype(BF16).astype(F32)
    for h in range(heads):
        one = q[:, h * head : (h + 1) * head]
        other = jnp.concatenate([one[:, head // 2 :], one[:, : head // 2]], -1)
        qs[:, h, :] = one * cos[...] + other * sin[...]

    own = lax.rem(lax.broadcasted_iota(jnp.int32, (qs.shape[1], 128), 1), heads) == lax.rem(lax.broadcasted_iota(jnp.int32, (qs.shape[1], 128), 0), heads)

    def score(s, out):
        out[...] = lax.dot_general(qs[s].astype(BF16), kb[lax.rem(s, slots)], (((1,), (1,)), ((), ())), preferred_element_type=F32)

    def weigh(s, given):
        pieces = [jnp.where(own, given[:, pl.ds(i * 128, 128)] * scale, -jnp.inf) for i in range(span // 128)]
        top = functools.reduce(jnp.maximum, pieces)
        top = jnp.max(top, -1, keepdims=True)
        pieces = [jnp.exp(p - top) for p in pieces]
        total = functools.reduce(jnp.add, pieces)
        share = 1.0 / jnp.sum(total, -1, keepdims=True)
        weights = jnp.concatenate([(p * share).astype(BF16) for p in pieces], -1)
        os[s] = dot(weights, vb[lax.rem(s, slots)])

    def refill(piece, s):
        @pl.when(s + slots < rows)
        def _():
            piece(s + slots).start()

    k_piece(0).wait()
    score(0, scores[0])
    refill(k_piece, jnp.int32(0))

    def steps(base, count, more):
        for i in range(count):
            if i + 1 < count or more:
                k_piece(base + i + 1).wait()
            v_piece(base + i).wait()
        for i in range(count):
            if i + 1 < count or more:
                score(base + i + 1, scores[(i + 1) % 2])
            weigh(base + i, scores[i % 2])
        for i in range(count):
            if more:
                refill(k_piece, base + i + 1)
                refill(v_piece, base + i)

    @pl.loop(0, rows // GROUP - 1)
    def _(j):
        steps(j * GROUP, GROUP, True)

    steps(jnp.int32(rows - GROUP), GROUP, False)
    for h in range(heads):
        seen[:, pl.ds(h * head, head)] = os[:, h, :].astype(BF16)


def attention(x, k_cache, v_cache, gain, wq):
    rows, cache, heads, head = k_cache.shape
    d, out = wq.shape
    half = head // 2
    angle = (cache - 1) * float(THETA) ** (-np.arange(half) / half)
    cos, sin = np.cos(angle), np.sin(angle)
    turn = [np.concatenate(pair)[None].astype(np.float32) for pair in ((cos, cos), (-sin, sin))]
    span = cache * heads
    pad = -(-heads // 8) * 8
    hbm, vmem, dma = pl.BlockSpec(memory_space=pl.ANY), pl.BlockSpec(memory_space=pltpu.VMEM), pltpu.SemaphoreType.DMA
    return pl.pallas_call(
        functools.partial(head_kernel, heads),
        out_shape=jax.ShapeDtypeStruct((rows, out), BF16),
        in_specs=[hbm, vmem, vmem, vmem, hbm, hbm, hbm],
        out_specs=vmem,
        scratch_shapes=[
            pltpu.VMEM((rows, d), BF16),
            pltpu.VMEM((rows, d), BF16),
            pltpu.VMEM((d, out), BF16),
            pltpu.VMEM((KV_SLOTS, span, head), BF16),
            pltpu.VMEM((KV_SLOTS, span, head), BF16),
            pltpu.VMEM((d // 128, 128), F32),
            pltpu.VMEM((rows, pad, head), F32),
            pltpu.VMEM((rows, pad, head), F32),
            pltpu.VMEM((pad, span), F32),
            pltpu.VMEM((pad, span), F32),
            dma,
            dma((8,)),
            dma((KV_SLOTS,)),
            dma((KV_SLOTS,)),
        ],
        compiler_params=pltpu.CompilerParams(vmem_limit_bytes=67043328),
        cost_estimate=pl.CostEstimate(flops=4 * rows * span * head * heads, bytes_accessed=4 * rows * span * head, transcendentals=0),
    )(x, gain.reshape(d // 128, 128), *turn, wq, k_cache.reshape(rows * span, head), v_cache.reshape(rows * span, head))


def tail_kernel(side, seen, x, gain, wo, w_gate, w_up, w_down, out, wg, wu, dn, xp, hp, term, own1, got1, sent2, own2, got2, ag, gf, b, gacc, uacc, hid,
                x_sem, wo_sem, g_sem, u_sem, d_sem, s1, r1, s2, r2, sv, rv, su, ru):
    me = lax.axis_index("tp")
    at = (me // side, me % side)
    rows, depth = seen.shape
    d, ff = w_gate.shape
    wide = d // (2 * side)
    w = wide // side
    bk = depth
    bn = wide // 2
    nk = d // bk
    order = FAR_FIRST + (0,)
    steps = [(g, h) for g in order for h in range(2)]

    def peer(axis, g):
        place = [at[0], at[1]]
        place[axis] = lax.rem(at[axis] + g, side)
        return {"tp": place[0] * side + place[1]}

    def first_column(h, g):
        return pl.multiple_of((h * side + lax.rem(at[h] + g, side)) * wide, wide)

    across = ff // bn
    wo_rows = -(-2 * len(steps) // across)

    def wo_piece(j):
        g, h = steps[j // 2]
        home = wu.at[pl.ds((nk - wo_rows + j // across) * bk, bk), pl.ds((j % across) * bn, bn)]
        return pltpu.make_async_copy(wo.at[:, pl.ds(pl.multiple_of(first_column(h, g) + (j % 2) * bn, bn), bn)], home, wo_sem.at[j]), home

    def gate_piece(k):
        part = pl.ds(pl.multiple_of(k * bk, bk), bk)
        return pltpu.make_async_copy(w_gate.at[part, :], wg.at[part, :], g_sem.at[k])

    def up_piece(k):
        part = pl.ds(pl.multiple_of(k * bk, bk), bk)
        return pltpu.make_async_copy(w_up.at[part, :], wu.at[part, :], u_sem.at[k])

    def down_piece(j):
        g, h = steps[j // 2]
        return pltpu.make_async_copy(w_down.at[:, pl.ds(pl.multiple_of(first_column(h, g) + (j % 2) * bn, bn), bn)], dn.at[j % SLOTS], d_sem.at[j % SLOTS])

    def x_piece(h):
        return pltpu.make_async_copy(x.at[:, pl.ds(pl.multiple_of(first_column(h, 0) + at[1 - h] * w, w), w)], xp.at[h], x_sem.at[h])

    barrier = pltpu.get_barrier_semaphore()
    for axis in range(2):
        for g in range(1, side):
            pl.semaphore_signal(barrier, inc=1, device_id=peer(axis, g), device_id_type=MESH)
    for j in range(2 * len(steps)):
        wo_piece(j)[0].start()
    for h in range(2):
        x_piece(h).start()
    for k in range(nk):
        gate_piece(k).start()
        if k < nk - wo_rows:
            up_piece(k).start()
    for j in range(SLOTS):
        down_piece(j).start()
    pl.semaphore_wait(barrier, 2 * (side - 1))

    def summed(piece, base):
        firsts, seconds, copies = [], [], []
        for i, (g, h) in enumerate(steps):
            for c in range(2):
                value = piece(2 * i + c)
                if g:
                    term[h, g - 1, :, pl.ds(c * bn, bn)] = value.astype(BF16)
                else:
                    own1[h, :, pl.ds(c * bn, bn)] = value
            if g:
                copy = pltpu.make_async_remote_copy(term.at[h, g - 1], got1.at[h, g - 1], s1.at[h, g - 1], r1.at[h, g - 1], device_id=peer(h, g), device_id_type=MESH)
                copy.start()
                firsts.append((h, copy))
        for h in range(2):
            for half, copy in firsts:
                if half == h:
                    copy.wait_recv()
            for g in order:
                part = pl.ds(pl.multiple_of(lax.rem(at[1 - h] + g, side) * w, w), w)
                total = own1[h, :, part]
                for k in range(side - 1):
                    total += got1[h, k, :, part].astype(F32)
                if g:
                    sent2[h, g - 1] = total.astype(BF16)
                    copy = pltpu.make_async_remote_copy(sent2.at[h, g - 1], got2.at[h, g - 1], s2.at[h, g - 1], r2.at[h, g - 1], device_id=peer(1 - h, g), device_id_type=MESH)
                    copy.start()
                    seconds.append((h, copy))
                else:
                    own2[h] = total
        news, arrivals = {}, []
        for h in range(2):
            for half, copy in seconds:
                if half == h:
                    copy.wait_recv()
            total = own2[h]
            for k in range(side - 1):
                total += got2[h, k].astype(F32)
            value = (base(h) + total).astype(BF16)
            hp[h] = value
            mine = ag.at[h, at[h], at[1 - h]]
            mine[...] = value
            for g in FAR_FIRST:
                copy = pltpu.make_async_remote_copy(mine, mine, sv.at[h, g - 1], rv.at[h, g - 1], device_id=peer(1 - h, g), device_id_type=MESH)
                copy.start()
                news[h, g] = copy
                copies.append(copy)
            for g in FAR_FIRST:
                copy = pltpu.make_async_remote_copy(mine, mine, su.at[h, g - 1, 0], ru.at[h, g - 1, 0], device_id=peer(h, g), device_id_type=MESH)
                copy.start()
                copies.append(copy)
                arrivals.append(copy)
        for k in (1, 3, 2):
            for h in range(2):
                news[h, k].wait_recv()
                came = ag.at[h, at[h], lax.rem(at[1 - h] + side - k, side)]
                for g in FAR_FIRST:
                    copy = pltpu.make_async_remote_copy(came, came, su.at[h, g - 1, k], ru.at[h, g - 1, k], device_id=peer(h, g), device_id_type=MESH)
                    copy.start()
                    copies.append(copy)
                    arrivals.append(copy)
        for copy in arrivals:
            copy.wait_recv()
        for _, copy in firsts + seconds:
            copy.wait_send()
        for copy in copies:
            copy.wait_send()

    def attention_term(j):
        copy, home = wo_piece(j)
        copy.wait()
        value = dot(seen[...], home[...])
        if j % across == across - 1 or j == 2 * len(steps) - 1:
            up_piece(nk - wo_rows + j // across).start()
        return value

    def of_x(h):
        x_piece(h).wait()
        return xp[h].astype(F32)

    summed(attention_term, of_x)

    squares = jnp.zeros((rows, w), F32)
    blocks = [(h, u, v) for h in range(2) for u in range(side) for v in range(side)]
    for h, u, v in blocks:
        value = ag[h, u, v].astype(F32)
        squares += value * value
    scale = lax.rsqrt(jnp.sum(squares, -1, keepdims=True) / d + 1e-6)
    gf[...] = gain[...].astype(F32)
    for i, (h, u, v) in enumerate(blocks):
        for c in range(w // 128):
            value = ag[h, u, v, :, pl.ds(c * 128, 128)].astype(F32)
            b[:, pl.ds(i * w + c * 128, 128)] = (value * scale * gf[pl.ds(i * (w // 128) + c, 1), :]).astype(BF16)

    gacc[...] = jnp.zeros_like(gacc)
    uacc[...] = jnp.zeros_like(uacc)

    @pl.loop(0, nk // JOINT)
    def _(m):
        for k in range(JOINT):
            gate_piece(m * JOINT + k).wait()
            up_piece(m * JOINT + k).wait()
        part = pl.ds(pl.multiple_of(m * JOINT * bk, JOINT * bk), JOINT * bk)
        gacc[...] += dot(b[:, part], wg[part, :])
        uacc[...] += dot(b[:, part], wu[part, :])

    gate = gacc[...]
    hid[...] = (gate * jax.nn.sigmoid(gate) * uacc[...]).astype(BF16)

    def mlp_term(j):
        down_piece(j).wait()
        value = dot(hid[...], dn[j % SLOTS])
        if j + SLOTS < 2 * len(steps):
            down_piece(j + SLOTS).start()
        return value

    summed(mlp_term, lambda h: hp[h].astype(F32))
    for i, (h, u, v) in enumerate(blocks):
        out[:, pl.ds(i * w, w)] = ag[h, u, v]


def tail(side, seen, x, gain, wo, w_gate, w_up, w_down):
    rows, depth = seen.shape
    d, ff = w_gate.shape
    wide = d // (2 * side)
    w = wide // side
    nk = d // depth
    hops = side - 1
    hbm, vmem, dma = pl.BlockSpec(memory_space=pl.ANY), pl.BlockSpec(memory_space=pltpu.VMEM), pltpu.SemaphoreType.DMA
    return pl.pallas_call(
        functools.partial(tail_kernel, side),
        out_shape=jax.ShapeDtypeStruct((rows, d), BF16),
        in_specs=[vmem, hbm, vmem, hbm, hbm, hbm, hbm],
        out_specs=vmem,
        scratch_shapes=[
            pltpu.VMEM((d, ff), BF16),
            pltpu.VMEM((d, ff), BF16),
            pltpu.VMEM((SLOTS, ff, wide // 2), BF16),
            pltpu.VMEM((2, rows, w), BF16),
            pltpu.VMEM((2, rows, w), BF16),
            pltpu.VMEM((2, hops, rows, wide), BF16),
            pltpu.VMEM((2, rows, wide), F32),
            pltpu.VMEM((2, hops, rows, wide), BF16),
            pltpu.VMEM((2, hops, rows, w), BF16),
            pltpu.VMEM((2, rows, w), F32),
            pltpu.VMEM((2, hops, rows, w), BF16),
            pltpu.VMEM((2, side, side, rows, w), BF16),
            pltpu.VMEM((d // 128, 128), F32),
            pltpu.VMEM((rows, d), BF16),
            pltpu.VMEM((rows, ff), F32),
            pltpu.VMEM((rows, ff), F32),
            pltpu.VMEM((rows, ff), BF16),
            dma((2,)),
            dma((4 * side,)),
            dma((nk,)),
            dma((nk,)),
            dma((SLOTS,)),
            dma((2, hops)),
            dma((2, hops)),
            dma((2, hops)),
            dma((2, hops)),
            dma((2, hops)),
            dma((2, hops)),
            dma((2, hops, side)),
            dma((2, hops, side)),
        ],
        compiler_params=pltpu.CompilerParams(collective_id=0, has_side_effects=True, vmem_limit_bytes=67043328),
    )(seen, x, gain.reshape(d // 128, 128), wo, w_gate, w_up, w_down)


def solution(mesh):
    side = math.isqrt(mesh.shape["tp"])

    def step(x, k_cache, v_cache, gain_a, wq, wo, gain_m, w_gate, w_up, w_down):
        seen = attention(x, k_cache, v_cache, gain_a, wq)
        return tail(side, seen, x, gain_m, wo, w_gate, w_up, w_down)

    states, cache, columns, rows_of = P("dp", None), P("dp", None, "tp", None), P(None, "tp"), P("tp", None)
    return jax.shard_map(
        step,
        mesh=mesh,
        in_specs=(states, cache, cache, P(None), columns, rows_of, P(None), columns, columns, rows_of),
        out_specs=states,
        check_vma=False,
    )
```

```python
import functools
import math

import jax
import jax.numpy as jnp
import numpy as np
from jax import lax
from jax.experimental import pallas as pl
from jax.experimental.pallas import tpu as pltpu
from jax.sharding import PartitionSpec as P

THETA = 10000
BF16, F32 = jnp.bfloat16, jnp.float32
MESH = pl.DeviceIdType.MESH
LANES = 128
SLOTS = 4
GROUP = 4
FIRST = 2
JOINT = 8
FAR_FIRST = (2, 1, 3)
SHORT = (False, False, True)
SHORT_LAST = True
CHUNKS = (4, 2, 2)
EVENTS = {8: [(0, 0)], 5: [(0, 1)], 4: [(1, 0)], 3: [(0, 2)], 2: [(1, 1)], 1: [(0, 3)], 0: [(2, 0), (1, 2), (2, 1), (1, 3), (2, 2), (0, 4), (2, 3), (1, 4), (2, 4)]}


def dot(a, w):
    return jnp.dot(a, w, preferred_element_type=F32)


def kernel(side, heads, x, gain_a, gain_m, cos, sin, wq, k, v, wo, w_gate, w_up, w_down, out,
           wg, wu, dn, term, own1, got1, sent2, own2, got2, partial, ag, gf, b, qs, os, sc0, sc1, seen, gacc, uacc, hid,
           x_sem, wq_sem, k_sem, v_sem, wo_sem, g_sem, u_sem, d_sem, s1, r1, s2, r2, sv, rv, su, ru):
    me = lax.axis_index("tp")
    at = (me // side, me % side)
    rows, d = x.shape
    head = k.shape[1]
    span = k.shape[0] // rows
    depth = heads * head
    ff = w_gate.shape[1]
    wide = d // (2 * side)
    w = wide // side
    bk = depth
    bn = wide // 2
    narrow = w // 2
    nk = d // bk
    order = FAR_FIRST + (0,)
    steps = [(g, h) for g in order for h in range(2)]
    pieces_of = [(c, h, u, t) for c in range(2) for h in range(2) for u in range(side) for t in range(side)]

    def peer(axis, g):
        place = [at[0], at[1]]
        place[axis] = lax.rem(at[axis] + g, side)
        return {"tp": place[0] * side + place[1]}

    def group(c, h, g):
        return pl.ds(pl.multiple_of(((c * 2 + h) * side + lax.rem(at[h] + g, side)) * bn, bn), bn)

    strips = (ff - depth) // LANES
    k_slots, v_slots = strips * (d // span), ff // LANES

    def k_home(s):
        i = lax.rem(s, k_slots)
        return pl.ds(pl.multiple_of(i // strips * span, span), span), pl.ds(pl.multiple_of(depth + lax.rem(i, strips) * LANES, LANES), LANES)

    def v_home(s):
        return pl.ds(0, span), pl.ds(pl.multiple_of(lax.rem(s, v_slots) * LANES, LANES), LANES)

    def k_piece(s):
        return pltpu.make_async_copy(k.at[pl.ds(pl.multiple_of(s * span, span), span), :], wg.at[k_home(s)], k_sem.at[lax.rem(s, k_slots)])

    def v_piece(s):
        return pltpu.make_async_copy(v.at[pl.ds(pl.multiple_of(s * span, span), span), :], wu.at[v_home(s)], v_sem.at[lax.rem(s, v_slots)])

    n_wq = wq_sem.shape[0]

    def wq_piece(i):
        part = pl.ds(i * (d // n_wq), d // n_wq)
        return pltpu.make_async_copy(wq.at[part, :], wg.at[part, pl.ds(0, depth)], wq_sem.at[i])

    across = ff // bn
    wo_rows = -(-2 * len(steps) // across)

    def wo_piece(j):
        g, h = steps[j // 2]
        home = wu.at[pl.ds((nk - wo_rows + j // across) * bk, bk), pl.ds((j % across) * bn, bn)]
        return pltpu.make_async_copy(wo.at[:, group(j % 2, h, g)], home, wo_sem.at[j]), home

    def gate_piece(i):
        part = pl.ds(pl.multiple_of(i * bk, bk), bk)
        return pltpu.make_async_copy(w_gate.at[part, :], wg.at[part, :], g_sem.at[i])

    def up_piece(i):
        part = pl.ds(pl.multiple_of(i * bk, bk), bk)
        return pltpu.make_async_copy(w_up.at[part, :], wu.at[part, :], u_sem.at[i])

    def down_piece(j):
        c, (g, h) = j // len(steps), steps[j % len(steps)]
        if j < SLOTS:
            home = dn.at[j]
        else:
            m, i = divmod(j - SLOTS, 2 * across)
            home = (wg, wu)[i // across].at[pl.ds(m * JOINT * bk, ff), pl.ds(i % across * bn, bn)]
        return pltpu.make_async_copy(w_down.at[:, group(c, h, g)], home, d_sem.at[j]), home

    def x_piece(i):
        c, h, u, t = pieces_of[i]
        return pltpu.make_async_copy(x.at[:, pl.ds(i * narrow, narrow)], ag.at[h, u, t, :, pl.ds(c * narrow, narrow)], x_sem.at[i])

    for i in range(len(pieces_of)):
        x_piece(i).start()
    barrier = pltpu.get_barrier_semaphore()
    for axis in range(2):
        for g in range(1, side):
            pl.semaphore_signal(barrier, inc=1, device_id=peer(axis, g), device_id_type=MESH)
    for i in range(n_wq):
        wq_piece(i).start()
    for s in range(FIRST):
        k_piece(jnp.int32(s)).start()
        v_piece(jnp.int32(s)).start()
    qs[...] = jnp.zeros_like(qs)
    for i in range(len(pieces_of)):
        x_piece(i).wait()

    def norm(gain):
        gf[...] = gain[...].astype(F32)
        squares = jnp.zeros((rows, narrow), F32)
        for c, h, u, t in pieces_of:
            value = ag[h, u, t, :, pl.ds(c * narrow, narrow)].astype(F32)
            squares += value * value
        scale = lax.rsqrt(jnp.sum(squares, -1, keepdims=True) / d + 1e-6)
        for i, (c, h, u, t) in enumerate(pieces_of):
            value = ag[h, u, t, :, pl.ds(c * narrow, narrow)].astype(F32)
            b[:, pl.ds(i * narrow, narrow)] = (value * scale * gf[pl.ds(i, 1), :]).astype(BF16)

    norm(gain_a)
    q = jnp.zeros((rows, depth), F32)
    for i in range(n_wq):
        if i == n_wq // 2:
            for s in range(FIRST, k_slots):
                k_piece(jnp.int32(s)).start()
                if s < v_slots:
                    v_piece(jnp.int32(s)).start()
        wq_piece(i).wait()
        part = pl.ds(i * (d // n_wq), d // n_wq)
        q += dot(b[:, part], wg[part, pl.ds(0, depth)])
    q = q.astype(BF16).astype(F32)
    for h in range(heads):
        one = q[:, h * head : (h + 1) * head]
        other = jnp.concatenate([one[:, head // 2 :], one[:, : head // 2]], -1)
        qs[:, h, :] = one * cos[...] + other * sin[...]

    pad = qs.shape[1]
    own = lax.rem(lax.broadcasted_iota(jnp.int32, (pad, LANES), 1), heads) == lax.rem(lax.broadcasted_iota(jnp.int32, (pad, LANES), 0), heads)
    scores = (sc0, sc1)

    def score(s, to):
        to[...] = lax.dot_general(qs[s].astype(BF16), wg[k_home(s)], (((1,), (1,)), ((), ())), preferred_element_type=F32)

    def weigh(s, given):
        pieces = [jnp.where(own, given[:, pl.ds(i * LANES, LANES)] * head**-0.5, -jnp.inf) for i in range(span // LANES)]
        top = jnp.max(functools.reduce(jnp.maximum, pieces), -1, keepdims=True)
        pieces = [jnp.exp(p - top) for p in pieces]
        share = 1.0 / jnp.sum(functools.reduce(jnp.add, pieces), -1, keepdims=True)
        os[s] = dot(jnp.concatenate([(p * share).astype(BF16) for p in pieces], -1), wu[v_home(s)])

    def refill(piece, s):
        @pl.when(s < rows)
        def _():
            piece(s).start()

    def attend(base, more):
        for i in range(GROUP):
            if i + 1 < GROUP or more:
                k_piece(base + i + 1).wait()
            v_piece(base + i).wait()
        for i in range(GROUP):
            if i + 1 < GROUP or more:
                score(base + i + 1, scores[(i + 1) % 2])
            weigh(base + i, scores[i % 2])
        if more:
            for i in range(GROUP):
                refill(k_piece, base + i + 1 + k_slots)
                refill(v_piece, base + i + v_slots)

    class Sum:
        def __init__(self, chunk, r0, nr, cs, ready, piece, short):
            self.chunk, self.part, self.cs, self.ready, self.piece, self.short = chunk, pl.ds(r0, nr), cs, ready, piece, short
            self.group = pl.ds(cs[0] * bn, len(cs) * bn)
            self.block = pl.ds(cs[0] * narrow, len(cs) * narrow)
            self.firsts, self.seconds, self.copies, self.news, self.arrivals = [], [], [], {}, []

        def send(self, source, target, sems, index, device):
            index = (self.chunk,) + index
            copy = pltpu.make_async_remote_copy(source, target, sems[0].at[index], sems[1].at[index], device_id=device, device_id_type=MESH)
            copy.start()
            return copy

        def stage(self, which):
            if self.short:
                (self.terms, self.exchange, self.spread, lambda: None, self.finish)[which]()
            else:
                (self.terms, self.second, self.gather, self.forward, self.finish)[which]()

        def terms(self):
            part, columns = self.part, self.group
            self.ready()
            todo = [(g, h, c) for g, h in steps for c in self.cs]

            def flush(j, value):
                g, h, c = todo[j]
                if not g:
                    own1[h, part, pl.ds(c * bn, bn)] = value
                    return
                term[h, g - 1, part, pl.ds(c * bn, bn)] = value.astype(BF16)
                if c == self.cs[-1]:
                    self.firsts.append((h, self.send(term.at[h, g - 1, part, columns], got1.at[h, g - 1, part, columns], (s1, r1), (h, g - 1), peer(h, g))))

            value = self.piece(0)
            for j in range(1, len(todo)):
                later = self.piece(j)
                flush(j - 1, value)
                value = later
            flush(len(todo) - 1, value)

        def exchange(self):
            part = self.part
            for h in range(2):
                for half, copy in self.firsts:
                    if half == h:
                        copy.wait_recv()
                for c in self.cs:
                    for t in range(side):
                        columns = pl.ds(c * bn + t * narrow, narrow)
                        total = own1[h, part, columns]
                        for i in range(side - 1):
                            total += got1[h, i, part, columns].astype(F32)
                        partial[h, at[1 - h], part, columns] = total.astype(BF16)
                mine = partial.at[h, at[1 - h], part, self.group]
                for g in FAR_FIRST:
                    self.seconds.append((h, self.send(mine, mine, (s2, r2), (h, g - 1), peer(1 - h, g))))

        def spread(self):
            part = self.part
            for h in range(2):
                for half, copy in self.seconds:
                    if half == h:
                        copy.wait_recv()
                for c in self.cs:
                    for t in range(side):
                        columns, narrows = pl.ds(c * bn + t * narrow, narrow), pl.ds(c * narrow, narrow)
                        total = partial[h, 0, part, columns].astype(F32)
                        for i in range(1, side):
                            total += partial[h, i, part, columns].astype(F32)
                        ag[h, at[h], t, part, narrows] = (ag[h, at[h], t, part, narrows].astype(F32) + total).astype(BF16)
                mine = ag.at[h, at[h], :, part, self.block]
                for g in FAR_FIRST:
                    self.arrivals.append(self.send(mine, mine, (su, ru), (h, g - 1, 0), peer(h, g)))

        def second(self):
            part = self.part
            for h in range(2):
                for half, copy in self.firsts:
                    if half == h:
                        copy.wait_recv()
                for g in order:
                    for c in self.cs:
                        columns = pl.ds(pl.multiple_of(c * bn + lax.rem(at[1 - h] + g, side) * narrow, narrow), narrow)
                        total = own1[h, part, columns]
                        for i in range(side - 1):
                            total += got1[h, i, part, columns].astype(F32)
                        if g:
                            sent2[h, g - 1, part, pl.ds(c * narrow, narrow)] = total.astype(BF16)
                        else:
                            own2[h, part, pl.ds(c * narrow, narrow)] = total
                    if g:
                        mine = (h, g - 1, part, self.block)
                        self.seconds.append((h, self.send(sent2.at[mine], got2.at[mine], (s2, r2), (h, g - 1), peer(1 - h, g))))

        def gather(self):
            part, columns = self.part, self.block
            for h in range(2):
                for half, copy in self.seconds:
                    if half == h:
                        copy.wait_recv()
                total = own2[h, part, columns]
                for i in range(side - 1):
                    total += got2[h, i, part, columns].astype(F32)
                mine = ag.at[h, at[h], at[1 - h], part, columns]
                mine[...] = (mine[...].astype(F32) + total).astype(BF16)
                for g in FAR_FIRST:
                    self.news[h, g] = self.send(mine, mine, (sv, rv), (h, g - 1), peer(1 - h, g))
                    self.copies.append(self.news[h, g])
                for g in FAR_FIRST:
                    self.arrivals.append(self.send(mine, mine, (su, ru), (h, g - 1, 0), peer(h, g)))

        def forward(self):
            for i in (1, 3, 2):
                for h in range(2):
                    self.news[h, i].wait_recv()
                    came = ag.at[h, at[h], lax.rem(at[1 - h] + side - i, side), self.part, self.block]
                    for g in FAR_FIRST:
                        self.arrivals.append(self.send(came, came, (su, ru), (h, g - 1, i), peer(h, g)))

        def finish(self):
            for copy in self.arrivals:
                copy.wait_recv()
            for _, copy in self.firsts + self.seconds:
                copy.wait_send()
            for copy in self.copies + self.arrivals:
                copy.wait_send()

    starts = [rows // 8 * sum(CHUNKS[:i]) for i in range(len(CHUNKS))]

    def chunk_sum(c):
        r0, nr = starts[c], rows // 8 * CHUNKS[c]

        def ready():
            if c == 0:
                for j in range(2 * len(steps)):
                    wo_piece(j)[0].wait()

        def piece(j):
            return dot(seen[pl.ds(r0, nr), :], wo_piece(j)[1][...])

        return Sum(c, r0, nr, (0, 1), ready, piece, SHORT[c])

    sums = [chunk_sum(c) for c in range(len(CHUNKS))]

    def run(c, which):
        if which == 0:
            for h in range(heads):
                seen[sums[c].part, pl.ds(h * head, head)] = os[sums[c].part, h, :].astype(BF16)
            if c == 0:
                pl.semaphore_wait(barrier, 2 * (side - 1))
        sums[c].stage(which)
        if which == 0 and c == len(CHUNKS) - 1:
            for i in range(wo_rows):
                up_piece(nk - wo_rows + i).start()

    for j in range(2 * len(steps)):
        wo_piece(j)[0].start()
    k_piece(jnp.int32(0)).wait()
    score(jnp.int32(0), scores[0])
    refill(k_piece, jnp.int32(k_slots))
    groups = rows // GROUP
    early = nk // (d // span)
    begun = groups - k_slots // (d // span) // GROUP - 1
    done = 0
    for back in sorted(set(EVENTS) | {groups - 1 - begun}, reverse=True):
        last = groups - 1 - back
        if back:
            if last + 1 - done > 1:
                @pl.loop(done, last + 1)
                def _(j):
                    attend(j * GROUP, True)
            else:
                attend(jnp.int32(done * GROUP), True)
        else:
            for j in range(done, groups):
                attend(jnp.int32(j * GROUP), j + 1 < groups)
        done = last + 1
        if last == begun:
            for i in range(early):
                gate_piece(i).start()
            for i in range(span // bk, nk - wo_rows):
                up_piece(i).start()
        if not back:
            for i in range(max(nk - early, span // bk)):
                if i < nk - early:
                    gate_piece(early + i).start()
                if i < span // bk:
                    up_piece(i).start()
        for c, which in EVENTS.get(back, ()):
            run(c, which)
            if not back and which == 0:
                for j in range(SLOTS):
                    down_piece(j)[0].start()

    norm(gain_m)
    gacc[...] = jnp.zeros_like(gacc)
    uacc[...] = jnp.zeros_like(uacc)

    @pl.loop(0, nk // JOINT)
    def _(m):
        for i in range(JOINT):
            gate_piece(m * JOINT + i).wait()
            up_piece(m * JOINT + i).wait()
        part = pl.ds(pl.multiple_of(m * JOINT * bk, JOINT * bk), JOINT * bk)
        gacc[...] += dot(b[:, part], wg[part, :])
        uacc[...] += dot(b[:, part], wu[part, :])
        for n in range(-(-(2 * len(steps) - SLOTS) // (2 * across))):

            @pl.when(m == n)
            def _():
                for j in range(SLOTS + n * 2 * across, min(SLOTS + (n + 1) * 2 * across, 2 * len(steps))):
                    down_piece(j)[0].start()

    gate = gacc[...]
    hid[...] = (gate * jax.nn.sigmoid(gate) * uacc[...]).astype(BF16)

    def mlp_sum(c):
        def ready():
            for j in range(len(steps)):
                down_piece(c * len(steps) + j)[0].wait()

        def piece(j):
            return dot(hid[...], down_piece(c * len(steps) + j)[1][...])

        return Sum(c, 0, rows, (c,), ready, piece, SHORT_LAST)

    finals = [mlp_sum(c) for c in range(2)]
    for which in range(5):
        for total in finals:
            total.stage(which)
    for i, (c, h, u, t) in enumerate(pieces_of):
        out[:, pl.ds(i * narrow, narrow)] = ag[h, u, t, :, pl.ds(c * narrow, narrow)]


def layer(side, x, k_cache, v_cache, gain_a, wq, wo, gain_m, w_gate, w_up, w_down):
    rows, cache, heads, head = k_cache.shape
    d, depth = wq.shape
    ff = w_gate.shape[1]
    half = head // 2
    angle = (cache - 1) * float(THETA) ** (-np.arange(half) / half)
    cos, sin = np.cos(angle), np.sin(angle)
    turn = [np.concatenate(pair)[None].astype(np.float32) for pair in ((cos, cos), (-sin, sin))]
    span = cache * heads
    pad = -(-heads // 8) * 8
    wide = d // (2 * side)
    w = wide // side
    nk = d // depth
    hops = side - 1
    chunks = len(CHUNKS)
    hbm, vmem, dma = pl.BlockSpec(memory_space=pl.ANY), pl.BlockSpec(memory_space=pltpu.VMEM), pltpu.SemaphoreType.DMA
    gains = [gain.reshape(d // LANES, LANES) for gain in (gain_a, gain_m)]
    return pl.pallas_call(
        functools.partial(kernel, side, heads),
        out_shape=jax.ShapeDtypeStruct((rows, d), BF16),
        in_specs=[hbm] + [vmem] * 4 + [hbm] * 7,
        out_specs=vmem,
        scratch_shapes=[
            pltpu.VMEM((d, ff), BF16),
            pltpu.VMEM((d, ff), BF16),
            pltpu.VMEM((SLOTS, ff, wide // 2), BF16),
            pltpu.VMEM((2, hops, rows, wide), BF16),
            pltpu.VMEM((2, rows, wide), F32),
            pltpu.VMEM((2, hops, rows, wide), BF16),
            pltpu.VMEM((2, hops, rows, w), BF16),
            pltpu.VMEM((2, rows, w), F32),
            pltpu.VMEM((2, hops, rows, w), BF16),
            pltpu.VMEM((2, side, rows, wide), BF16),
            pltpu.VMEM((2, side, side, rows, w), BF16),
            pltpu.VMEM((d // LANES, LANES), F32),
            pltpu.VMEM((rows, d), BF16),
            pltpu.VMEM((rows, pad, head), F32),
            pltpu.VMEM((rows, pad, head), F32),
            pltpu.VMEM((pad, span), F32),
            pltpu.VMEM((pad, span), F32),
            pltpu.VMEM((rows, depth), BF16),
            pltpu.VMEM((rows, ff), F32),
            pltpu.VMEM((rows, ff), F32),
            pltpu.VMEM((rows, ff), BF16),
            dma((4 * side * side,)),
            dma((8,)),
            dma(((ff - depth) // LANES * (d // span),)),
            dma((ff // LANES,)),
            dma((4 * side,)),
            dma((nk,)),
            dma((nk,)),
            dma((4 * side,)),
            dma((chunks, 2, hops)),
            dma((chunks, 2, hops)),
            dma((chunks, 2, hops)),
            dma((chunks, 2, hops)),
            dma((chunks, 2, hops)),
            dma((chunks, 2, hops)),
            dma((chunks, 2, hops, side)),
            dma((chunks, 2, hops, side)),
        ],
        compiler_params=pltpu.CompilerParams(collective_id=0, has_side_effects=True, vmem_limit_bytes=67043328),
    )(x, *gains, *turn, wq, k_cache.reshape(rows * span, head), v_cache.reshape(rows * span, head), wo, w_gate, w_up, w_down)


def solution(mesh):
    side = math.isqrt(mesh.shape["tp"])
    states, cache, columns, rows_of = P("dp", None), P("dp", None, "tp", None), P(None, "tp"), P("tp", None)
    return jax.shard_map(
        functools.partial(layer, side),
        mesh=mesh,
        in_specs=(states, cache, cache, P(None), columns, rows_of, P(None), columns, columns, rows_of),
        out_specs=states,
        check_vma=False,
    )
```

```python
import functools
import math

import jax
import jax.numpy as jnp
import numpy as np
from jax import lax
from jax.experimental import pallas as pl
from jax.experimental.pallas import tpu as pltpu
from jax.sharding import PartitionSpec as P

THETA = 10000
BF16, F32 = jnp.bfloat16, jnp.float32
MESH = pl.DeviceIdType.MESH
LANES = 128
SLOTS = 4
GROUP = 4
FIRST = 2
JOINT = 4
FAR_FIRST = (2, 1, 3)
CHUNKS = (4, 2, 2)
EVENTS = {8: [(0, 0)], 5: [(0, 1)], 4: [(1, 0)], 3: [(0, 2)], 2: [(1, 1)], 0: [(2, 0), (2, 1), (1, 2), (2, 2), (0, 3), (1, 3), (2, 3)]}


def dot(a, w):
    return jnp.dot(a, w, preferred_element_type=F32)


def kernel(side, heads, x, gain_a, gain_m, cos, sin, wq, k, v, wo, w_gate, w_up, w_down, out,
           wg, wu, dn, term, own1, got1, partial, ag, gf, b, qs, os, sc0, sc1, seen, gacc, uacc, hid,
           x_sem, wq_sem, k_sem, v_sem, wo_sem, g_sem, u_sem, d_sem, s1, r1, s2, r2, s3, r3):
    me = lax.axis_index("tp")
    at = (me // side, me % side)
    rows, d = x.shape
    head = k.shape[1]
    span = k.shape[0] // rows
    depth = heads * head
    ff = w_gate.shape[1]
    wide = d // (2 * side)
    w = wide // side
    bk = depth
    bn = wide // 2
    narrow = w // 2
    nk = d // bk
    steps = [(g, h) for g in FAR_FIRST + (0,) for h in range(2)]
    pieces_of = [(c, h, u, t) for c in range(2) for h in range(2) for u in range(side) for t in range(side)]

    def peer(axis, g):
        place = [at[0], at[1]]
        place[axis] = lax.rem(at[axis] + g, side)
        return {"tp": place[0] * side + place[1]}

    def group(c, h, g):
        return pl.ds(pl.multiple_of(((c * 2 + h) * side + lax.rem(at[h] + g, side)) * bn, bn), bn)

    strips = (ff - depth) // LANES
    k_slots, v_slots = strips * (d // span), ff // LANES

    def k_home(s):
        i = lax.rem(s, k_slots)
        return pl.ds(pl.multiple_of(i // strips * span, span), span), pl.ds(pl.multiple_of(depth + lax.rem(i, strips) * LANES, LANES), LANES)

    def v_home(s):
        return pl.ds(0, span), pl.ds(pl.multiple_of(lax.rem(s, v_slots) * LANES, LANES), LANES)

    def k_piece(s):
        return pltpu.make_async_copy(k.at[pl.ds(pl.multiple_of(s * span, span), span), :], wg.at[k_home(s)], k_sem.at[lax.rem(s, k_slots)])

    def v_piece(s):
        return pltpu.make_async_copy(v.at[pl.ds(pl.multiple_of(s * span, span), span), :], wu.at[v_home(s)], v_sem.at[lax.rem(s, v_slots)])

    n_wq = wq_sem.shape[0]

    def wq_piece(i):
        part = pl.ds(i * (d // n_wq), d // n_wq)
        return pltpu.make_async_copy(wq.at[part, :], wg.at[part, pl.ds(0, depth)], wq_sem.at[i])

    across = ff // bn
    wo_rows = -(-2 * len(steps) // across)

    def wo_piece(j):
        g, h = steps[j // 2]
        home = wu.at[pl.ds((nk - wo_rows + j // across) * bk, bk), pl.ds((j % across) * bn, bn)]
        return pltpu.make_async_copy(wo.at[:, group(j % 2, h, g)], home, wo_sem.at[j]), home

    def gate_piece(i):
        part = pl.ds(pl.multiple_of(i * bk, bk), bk)
        return pltpu.make_async_copy(w_gate.at[part, :], wg.at[part, :], g_sem.at[i])

    def up_piece(i):
        part = pl.ds(pl.multiple_of(i * bk, bk), bk)
        return pltpu.make_async_copy(w_up.at[part, :], wu.at[part, :], u_sem.at[i])

    def down_piece(j):
        c, (g, h) = j // len(steps), steps[j % len(steps)]
        if j < SLOTS:
            home = dn.at[j]
        else:
            m, i = divmod(j - SLOTS, 2 * across)
            home = (wg, wu)[i // across].at[pl.ds(m * JOINT * bk, ff), pl.ds(i % across * bn, bn)]
        return pltpu.make_async_copy(w_down.at[:, group(c, h, g)], home, d_sem.at[j]), home

    def x_piece(i):
        c, h, u, t = pieces_of[i]
        return pltpu.make_async_copy(x.at[:, pl.ds(i * narrow, narrow)], ag.at[h, u, t, :, pl.ds(c * narrow, narrow)], x_sem.at[i])

    for i in range(len(pieces_of)):
        x_piece(i).start()
    barrier = pltpu.get_barrier_semaphore()
    for axis in range(2):
        for g in range(1, side):
            pl.semaphore_signal(barrier, inc=1, device_id=peer(axis, g), device_id_type=MESH)
    for i in range(n_wq):
        wq_piece(i).start()
    for s in range(FIRST):
        k_piece(jnp.int32(s)).start()
        v_piece(jnp.int32(s)).start()
    qs[...] = jnp.zeros_like(qs)
    for i in range(len(pieces_of)):
        x_piece(i).wait()

    def norm(gain):
        gf[...] = gain[...].astype(F32)
        squares = jnp.zeros((rows, narrow), F32)
        for c, h, u, t in pieces_of:
            value = ag[h, u, t, :, pl.ds(c * narrow, narrow)].astype(F32)
            squares += value * value
        scale = lax.rsqrt(jnp.sum(squares, -1, keepdims=True) / d + 1e-6)
        for i, (c, h, u, t) in enumerate(pieces_of):
            value = ag[h, u, t, :, pl.ds(c * narrow, narrow)].astype(F32)
            b[:, pl.ds(i * narrow, narrow)] = (value * scale * gf[pl.ds(i, 1), :]).astype(BF16)

    norm(gain_a)
    q = jnp.zeros((rows, depth), F32)
    for i in range(n_wq):
        if i == n_wq // 2:
            for s in range(FIRST, k_slots):
                k_piece(jnp.int32(s)).start()
                if s < v_slots:
                    v_piece(jnp.int32(s)).start()
        wq_piece(i).wait()
        part = pl.ds(i * (d // n_wq), d // n_wq)
        q += dot(b[:, part], wg[part, pl.ds(0, depth)])
    q = q.astype(BF16).astype(F32)
    for h in range(heads):
        one = q[:, h * head : (h + 1) * head]
        other = jnp.concatenate([one[:, head // 2 :], one[:, : head // 2]], -1)
        qs[:, h, :] = one * cos[...] + other * sin[...]

    pad = qs.shape[1]
    own = lax.rem(lax.broadcasted_iota(jnp.int32, (pad, LANES), 1), heads) == lax.rem(lax.broadcasted_iota(jnp.int32, (pad, LANES), 0), heads)
    scores = (sc0, sc1)

    def score(s, to):
        to[...] = lax.dot_general(qs[s].astype(BF16), wg[k_home(s)], (((1,), (1,)), ((), ())), preferred_element_type=F32)

    def weigh(s, given):
        pieces = [jnp.where(own, given[:, pl.ds(i * LANES, LANES)] * head**-0.5, -jnp.inf) for i in range(span // LANES)]
        top = jnp.max(functools.reduce(jnp.maximum, pieces), -1, keepdims=True)
        pieces = [jnp.exp(p - top) for p in pieces]
        share = 1.0 / jnp.sum(functools.reduce(jnp.add, pieces), -1, keepdims=True)
        os[s] = dot(jnp.concatenate([(p * share).astype(BF16) for p in pieces], -1), wu[v_home(s)])

    def refill(piece, s):
        @pl.when(s < rows)
        def _():
            piece(s).start()

    def attend(base, more):
        for i in range(GROUP):
            if i + 1 < GROUP or more:
                k_piece(base + i + 1).wait()
            v_piece(base + i).wait()
        for i in range(GROUP):
            if i + 1 < GROUP or more:
                score(base + i + 1, scores[(i + 1) % 2])
            weigh(base + i, scores[i % 2])
        if more:
            for i in range(GROUP):
                refill(k_piece, base + i + 1 + k_slots)
                refill(v_piece, base + i + v_slots)

    class Sum:
        def __init__(self, chunk, r0, nr, cs, ready, piece):
            self.chunk, self.part, self.cs, self.ready, self.piece = chunk, pl.ds(r0, nr), cs, ready, piece
            self.group = pl.ds(cs[0] * bn, len(cs) * bn)
            self.block = pl.ds(cs[0] * narrow, len(cs) * narrow)
            self.firsts, self.seconds, self.arrivals = [], [], []

        def send(self, source, target, sems, index, device):
            index = (self.chunk,) + index
            copy = pltpu.make_async_remote_copy(source, target, sems[0].at[index], sems[1].at[index], device_id=device, device_id_type=MESH)
            copy.start()
            return copy

        def stage(self, which):
            (self.terms, self.exchange, self.spread, self.finish)[which]()

        def terms(self):
            part, columns = self.part, self.group
            self.ready()
            todo = [(g, h, c) for g, h in steps for c in self.cs]

            def flush(j, value):
                g, h, c = todo[j]
                if not g:
                    own1[h, part, pl.ds(c * bn, bn)] = value
                    return
                term[h, g - 1, part, pl.ds(c * bn, bn)] = value.astype(BF16)
                if c == self.cs[-1]:
                    self.firsts.append((h, self.send(term.at[h, g - 1, part, columns], got1.at[h, g - 1, part, columns], (s1, r1), (h, g - 1), peer(h, g))))

            value = self.piece(0)
            for j in range(1, len(todo)):
                later = self.piece(j)
                flush(j - 1, value)
                value = later
            flush(len(todo) - 1, value)

        def exchange(self):
            part = self.part
            for h in range(2):
                for half, copy in self.firsts:
                    if half == h:
                        copy.wait_recv()
                for c in self.cs:
                    for t in range(side):
                        columns = pl.ds(c * bn + t * narrow, narrow)
                        total = own1[h, part, columns]
                        for i in range(side - 1):
                            total += got1[h, i, part, columns].astype(F32)
                        partial[h, at[1 - h], part, columns] = total.astype(BF16)
                mine = partial.at[h, at[1 - h], part, self.group]
                for g in FAR_FIRST:
                    self.seconds.append((h, self.send(mine, mine, (s2, r2), (h, g - 1), peer(1 - h, g))))

        def spread(self):
            part = self.part
            for h in range(2):
                for half, copy in self.seconds:
                    if half == h:
                        copy.wait_recv()
                for c in self.cs:
                    for t in range(side):
                        columns, narrows = pl.ds(c * bn + t * narrow, narrow), pl.ds(c * narrow, narrow)
                        total = partial[h, 0, part, columns].astype(F32)
                        for i in range(1, side):
                            total += partial[h, i, part, columns].astype(F32)
                        ag[h, at[h], t, part, narrows] = (ag[h, at[h], t, part, narrows].astype(F32) + total).astype(BF16)
                mine = ag.at[h, at[h], :, part, self.block]
                for g in FAR_FIRST:
                    self.arrivals.append(self.send(mine, mine, (s3, r3), (h, g - 1), peer(h, g)))

        def finish(self):
            for copy in self.arrivals:
                copy.wait_recv()
            for _, copy in self.firsts + self.seconds:
                copy.wait_send()
            for copy in self.arrivals:
                copy.wait_send()

    starts = [rows // 8 * sum(CHUNKS[:i]) for i in range(len(CHUNKS))]

    def chunk_sum(c):
        r0, nr = starts[c], rows // 8 * CHUNKS[c]

        def ready():
            if c == 0:
                for j in range(2 * len(steps)):
                    wo_piece(j)[0].wait()

        def piece(j):
            return dot(seen[pl.ds(r0, nr), :], wo_piece(j)[1][...])

        return Sum(c, r0, nr, (0, 1), ready, piece)

    sums = [chunk_sum(c) for c in range(len(CHUNKS))]

    def run(c, which):
        if which == 0:
            for h in range(heads):
                seen[sums[c].part, pl.ds(h * head, head)] = os[sums[c].part, h, :].astype(BF16)
            if c == 0:
                pl.semaphore_wait(barrier, 2 * (side - 1))
        sums[c].stage(which)
        if which == 0 and c == len(CHUNKS) - 1:
            for i in range(wo_rows):
                up_piece(nk - wo_rows + i).start()

    for j in range(2 * len(steps)):
        wo_piece(j)[0].start()
    k_piece(jnp.int32(0)).wait()
    score(jnp.int32(0), scores[0])
    refill(k_piece, jnp.int32(k_slots))
    groups = rows // GROUP
    early = nk // (d // span)
    begun = groups - k_slots // (d // span) // GROUP - 1
    done = 0
    for back in sorted(set(EVENTS) | {groups - 1 - begun}, reverse=True):
        last = groups - 1 - back
        if back:
            if last + 1 - done > 1:
                @pl.loop(done, last + 1)
                def _(j):
                    attend(j * GROUP, True)
            else:
                attend(jnp.int32(done * GROUP), True)
        else:
            for j in range(done, groups):
                attend(jnp.int32(j * GROUP), j + 1 < groups)
        done = last + 1
        if last == begun:
            for i in range(early):
                gate_piece(i).start()
            for i in range(span // bk, nk - wo_rows):
                up_piece(i).start()
        if not back:
            for i in range(max(nk - early, span // bk)):
                if i < nk - early:
                    gate_piece(early + i).start()
                if i < span // bk:
                    up_piece(i).start()
        for c, which in EVENTS.get(back, ()):
            run(c, which)
            if not back and which == 0:
                for j in range(SLOTS):
                    down_piece(j)[0].start()

    norm(gain_m)
    gacc[...] = jnp.zeros_like(gacc)
    uacc[...] = jnp.zeros_like(uacc)

    @pl.loop(0, nk // JOINT)
    def _(m):
        for i in range(JOINT):
            gate_piece(m * JOINT + i).wait()
            up_piece(m * JOINT + i).wait()
        part = pl.ds(pl.multiple_of(m * JOINT * bk, JOINT * bk), JOINT * bk)
        gacc[...] += dot(b[:, part], wg[part, :])
        uacc[...] += dot(b[:, part], wu[part, :])
        for n in range(-(-(2 * len(steps) - SLOTS) // (2 * across))):

            @pl.when(m == n)
            def _():
                for j in range(SLOTS + n * 2 * across, min(SLOTS + (n + 1) * 2 * across, 2 * len(steps))):
                    down_piece(j)[0].start()

    gate = gacc[...]
    hid[...] = (gate * jax.nn.sigmoid(gate) * uacc[...]).astype(BF16)

    def mlp_sum(c):
        def ready():
            for j in range(len(steps)):
                down_piece(c * len(steps) + j)[0].wait()

        def piece(j):
            return dot(hid[...], down_piece(c * len(steps) + j)[1][...])

        return Sum(c, 0, rows, (c,), ready, piece)

    finals = [mlp_sum(c) for c in range(2)]
    for which in range(4):
        for total in finals:
            total.stage(which)
    for i, (c, h, u, t) in enumerate(pieces_of):
        out[:, pl.ds(i * narrow, narrow)] = ag[h, u, t, :, pl.ds(c * narrow, narrow)]


def layer(side, x, k_cache, v_cache, gain_a, wq, wo, gain_m, w_gate, w_up, w_down):
    rows, cache, heads, head = k_cache.shape
    d, depth = wq.shape
    ff = w_gate.shape[1]
    half = head // 2
    angle = (cache - 1) * float(THETA) ** (-np.arange(half) / half)
    cos, sin = np.cos(angle), np.sin(angle)
    turn = [np.concatenate(pair)[None].astype(np.float32) for pair in ((cos, cos), (-sin, sin))]
    span = cache * heads
    pad = -(-heads // 8) * 8
    wide = d // (2 * side)
    w = wide // side
    nk = d // depth
    hops = side - 1
    chunks = len(CHUNKS)
    hbm, vmem, dma = pl.BlockSpec(memory_space=pl.ANY), pl.BlockSpec(memory_space=pltpu.VMEM), pltpu.SemaphoreType.DMA
    gains = [gain.reshape(d // LANES, LANES) for gain in (gain_a, gain_m)]
    return pl.pallas_call(
        functools.partial(kernel, side, heads),
        out_shape=jax.ShapeDtypeStruct((rows, d), BF16),
        in_specs=[hbm] + [vmem] * 4 + [hbm] * 7,
        out_specs=vmem,
        scratch_shapes=[
            pltpu.VMEM((d, ff), BF16),
            pltpu.VMEM((d, ff), BF16),
            pltpu.VMEM((SLOTS, ff, wide // 2), BF16),
            pltpu.VMEM((2, hops, rows, wide), BF16),
            pltpu.VMEM((2, rows, wide), F32),
            pltpu.VMEM((2, hops, rows, wide), BF16),
            pltpu.VMEM((2, side, rows, wide), BF16),
            pltpu.VMEM((2, side, side, rows, w), BF16),
            pltpu.VMEM((d // LANES, LANES), F32),
            pltpu.VMEM((rows, d), BF16),
            pltpu.VMEM((rows, pad, head), F32),
            pltpu.VMEM((rows, pad, head), F32),
            pltpu.VMEM((pad, span), F32),
            pltpu.VMEM((pad, span), F32),
            pltpu.VMEM((rows, depth), BF16),
            pltpu.VMEM((rows, ff), F32),
            pltpu.VMEM((rows, ff), F32),
            pltpu.VMEM((rows, ff), BF16),
            dma((4 * side * side,)),
            dma((8,)),
            dma(((ff - depth) // LANES * (d // span),)),
            dma((ff // LANES,)),
            dma((4 * side,)),
            dma((nk,)),
            dma((nk,)),
            dma((4 * side,)),
            dma((chunks, 2, hops)),
            dma((chunks, 2, hops)),
            dma((chunks, 2, hops)),
            dma((chunks, 2, hops)),
            dma((chunks, 2, hops)),
            dma((chunks, 2, hops)),
        ],
        compiler_params=pltpu.CompilerParams(collective_id=0, has_side_effects=True, vmem_limit_bytes=67043328),
    )(x, *gains, *turn, wq, k_cache.reshape(rows * span, head), v_cache.reshape(rows * span, head), wo, w_gate, w_up, w_down)


def solution(mesh):
    side = math.isqrt(mesh.shape["tp"])
    states, cache, columns, rows_of = P("dp", None), P("dp", None, "tp", None), P(None, "tp"), P("tp", None)
    return jax.shard_map(
        functools.partial(layer, side),
        mesh=mesh,
        in_specs=(states, cache, cache, P(None), columns, rows_of, P(None), columns, columns, rows_of),
        out_specs=states,
        check_vma=False,
    )
```
